32 devices in a mesh: frag: 2 (over y), gx: 16 (over z, x, core).
Axes of the slice: x: 2, y: 2, z: 4, core: 2. Of those that a mesh axis runs over, the one named last changes fastest.
Arguments:
- coefficient: float32 [16384], P(('frag', 'gx')), parts along dimension 0, may hold values from 0.05 to 0.3
- exponent: float32 [16384], P(('frag', 'gx')), parts along dimension 0, may hold values from 0.05 to 0.5
- centers: float32 [3, 16384], P(None, ('frag', 'gx')), parts along dimension 1, may hold values from -2 to 2
- density: float32 [16384], P(('frag', 'gx')), parts along dimension 0, may hold values from -6 to 6
- core_fock: float32 [16384], P(('frag', 'gx')), parts along dimension 0, may hold values from -6 to 6
- shell_ang: int32 [64], P('frag'), parts along dimension 0, may hold values from 0 to 3, as said below
- tile_list: int32 [2, 4096], P(None, ('frag', 'gx')), parts along dimension 1, may hold values from 0 to 31, as said below
Outputs:
- fock: float32 [16384], P(('frag', 'gx')), parts along dimension 0
The draws below stay inside these ranges and needn't reach their ends.
There are 2 independent parts, one for each index of `frag`. The reference program is written for one: setup_inputs(seed, part) draws one part's arguments, and reference() takes and returns one part's arrays. A program takes and returns all parts, laid end to end along the dimension named above; each array names one. Nothing has to cross between parts.
Inputs may be any that keep to these rules, and one draw needn't show every extreme that they name: `shell_ang`: each of 0 to 3 is the angular momentum of exactly 8 blocks; blocks 0 to 1 all have 0. `tile_list`: kind never falls along the list, and kinds 0 to 6 fill 1, 2, 3, 4, 3, 2, 1 sixteenths of the list in turn; pair block b is owned by index b // 2 of gx; among the 128 tiles of one index of gx at most 32 have bra blocks of one owner, and index 0 of gx holds exactly 32 tiles for owner 0.
All inputs are finite; a program needn't handle non-finite values.
Results may differ from the reference program's by a relative error of at most 0.0003.
Values sent between devices are 32-bit elements; how exact they have to be, the bound alone decides.
No kernel may reach another device: no remote copies, remote signals or barrier semaphores. Data moves between devices by JAX's collectives and lax.ppermute only.
A program may use at most 128 MiB of HBM per device.

```python
import math
import jax
import jax.numpy as jnp
from jax import lax

PB = 256
MAXL = 3
BLK_DEV = 2
TILE_DEV = 128
NBLK = 32
NPAIR = 8192
NTILE = 2048


def shared_ang(key):
    levels = jnp.sort(jnp.arange(NBLK, dtype=jnp.int32) % (MAXL + 1))
    remaining = levels[BLK_DEV:]
    mixed = remaining[jax.random.permutation(jax.random.fold_in(key, 11), NBLK - BLK_DEV)]
    return jnp.concatenate([jnp.zeros((BLK_DEV,), jnp.int32), mixed]).astype(jnp.int32)


def draw_shell_ang(key, part):
    return shared_ang(key)


def draw_tile_list(key, part):
    angular = shared_ang(key)
    kinds_count = 2 * MAXL + 1
    sixteenth = NTILE // 16
    shares = jnp.array([1, 2, 3, 4, 3, 2, 1], jnp.int32)
    bounds = jnp.cumsum(shares) * sixteenth
    starts = bounds - shares * sixteenth
    position = jnp.arange(NTILE, dtype=jnp.int32)
    kind = jnp.sum((position[:, None] >= bounds[None, :]).astype(jnp.int32), axis=1).astype(jnp.int32)
    device = (position // TILE_DEV).astype(jnp.int32)
    run_start = jnp.maximum(device * TILE_DEV, starts[kind])
    rank_in_run = position - run_start
    orders = []
    sizes = []
    for kind_value in range(kinds_count):
        lowest = max(0, kind_value - MAXL)
        highest = min(MAXL, kind_value)
        eligible = (angular >= lowest) & (angular <= highest)
        ranks = jax.random.permutation(jax.random.fold_in(key, 20 + kind_value), NBLK).astype(jnp.int32)
        scores = jnp.where(eligible, ranks, NBLK + ranks)
        orders.append(jnp.argsort(scores).astype(jnp.int32))
        sizes.append((highest - lowest + 1) * (NBLK // (MAXL + 1)))
    orders = jnp.stack(orders)
    sizes = jnp.array(sizes, jnp.int32)
    offsets = jax.random.randint(jax.random.fold_in(key, 30), (NTILE // TILE_DEV, kinds_count), 0, NBLK).astype(jnp.int32)
    chosen = (offsets[device, kind] + rank_in_run) % sizes[kind]
    bra_block = orders[kind, chosen].astype(jnp.int32)
    lists = []
    for level in range(MAXL + 1):
        ranks = jax.random.permutation(jax.random.fold_in(key, 40 + level), NBLK).astype(jnp.int32)
        scores = jnp.where(angular == level, ranks, NBLK + ranks)
        lists.append(jnp.argsort(scores).astype(jnp.int32))
    lists = jnp.stack(lists)
    needed = (kind - angular[bra_block]).astype(jnp.int32)
    picks = jax.random.randint(jax.random.fold_in(key, 50), (NTILE,), 0, NBLK // (MAXL + 1)).astype(jnp.int32)
    ket_block = lists[needed, picks].astype(jnp.int32)
    return jnp.stack([bra_block, ket_block]).astype(jnp.int32)


def block_scale(stream_key, extent, shards, smallest, high):
    def one(axis_at, shards_of):
        draws = jax.random.uniform(jax.random.fold_in(jax.random.fold_in(stream_key, 6), axis_at), (shards_of,), jnp.float32, smallest / len(shards), high / len(shards))
        return jnp.repeat(jnp.exp(draws), extent[axis_at] // shards_of).reshape((-1,) + (1,) * (len(extent) - axis_at - 1))

    loudness = one(*shards[0])
    for cut in shards[1:]:
        loudness = loudness * one(*cut)
    return loudness


def centred(stream_key, dims, scale, limit, pieces=(), kind=jnp.bfloat16):
    gain = block_scale(stream_key, dims, pieces, -0.22, 0.18) if pieces else 1.0
    entries = jax.random.normal(stream_key, dims, jnp.float32) * scale * gain
    return jnp.minimum(jnp.maximum(entries, -limit), limit).astype(kind)


def setup_inputs(seed: int = 0, part: int = 0) -> dict:
    keys = jax.random.split(jax.random.key(seed), 8)
    own_keys = jax.random.split(jax.random.fold_in(keys[7], part), 8)
    return {
        "coefficient": jnp.clip(jnp.exp(math.log(0.3) - 1.7917595 * jax.random.uniform(own_keys[0], (NPAIR,), jnp.float32) ** block_scale(own_keys[0], (NPAIR,), ((0, 16),), -0.2, 0.2)), 0.05, 0.3),
        "exponent": jnp.clip(jnp.exp(math.log(0.5) - 2.3025851 * jax.random.uniform(own_keys[1], (NPAIR,), jnp.float32) ** block_scale(own_keys[1], (NPAIR,), ((0, 16),), -0.2, 0.2)), 0.05, 0.5),
        "centers": jnp.clip(jax.random.uniform(own_keys[2], (3, NPAIR), jnp.float32, -2.0, 2.0) * block_scale(own_keys[2], (3, NPAIR), ((1, 16),), -0.4, 0.0), -2.0, 2.0),
        "density": centred(own_keys[3], (NPAIR,), 1.0, 6.0, ((0, 16),), jnp.float32),
        "core_fock": centred(own_keys[4], (NPAIR,), 1.0, 6.0, ((0, 16),), jnp.float32),
        "shell_ang": draw_shell_ang(jax.random.fold_in(jax.random.fold_in(keys[7], part), 71), part),
        "tile_list": draw_tile_list(jax.random.fold_in(jax.random.fold_in(keys[7], part), 71), part),
    }


def pair_series(bra_exp, bra_cen, ket_exp, ket_cen, angular):
    distance = jnp.zeros((bra_exp.shape[0], bra_exp.shape[1], ket_exp.shape[1]), jnp.float32)
    for coordinate in range(3):
        offset = bra_cen[coordinate][:, :, None] - ket_cen[coordinate][:, None, :]
        distance = distance + offset * offset
    denominator = bra_exp[:, :, None] + ket_exp[:, None, :] + distance
    ratio = distance / denominator
    series_term = jnp.ones_like(ratio)
    series_sum = jnp.ones_like(ratio)
    for power in range(1, 2 * MAXL + 1):
        series_term = series_term * ratio
        series_sum = series_sum + jnp.where(power <= angular[:, None, None], series_term / (2 * power + 1), 0.0)
    return series_sum * lax.rsqrt(denominator)

def reference(coefficient, exponent, centers, density, core_fock, shell_ang, tile_list):
    coef_blocks = coefficient.reshape(NBLK, PB)
    exp_blocks = exponent.reshape(NBLK, PB)
    cen_blocks = centers.reshape(3, NBLK, PB)
    dens_blocks = density.reshape(NBLK, PB)
    angular = shell_ang[tile_list[0]] + shell_ang[tile_list[1]]
    group_size = 64

    def one_group(packed):
        bra_ids, ket_ids, kinds = packed
        kernel = pair_series(exp_blocks[bra_ids], cen_blocks[:, bra_ids], exp_blocks[ket_ids], cen_blocks[:, ket_ids], kinds)
        value = kernel * coef_blocks[bra_ids][:, :, None] * coef_blocks[ket_ids][:, None, :]
        return jnp.einsum('tij,tj->ti', value, dens_blocks[ket_ids], precision=lax.Precision.HIGHEST)
    partials = lax.map(one_group, (tile_list[0].reshape(-1, group_size), tile_list[1].reshape(-1, group_size), angular.reshape(-1, group_size)))
    coulomb = jnp.zeros((NBLK, PB), jnp.float32).at[tile_list[0]].add(partials.reshape(NTILE, PB))
    return core_fock + coulomb.reshape(NBLK * PB)
```

```python
import jax
import jax.numpy as jnp
from jax import lax
from jax.experimental import pallas as pl
from jax.experimental.pallas import tpu as pltpu
from jax.sharding import PartitionSpec as P

PB = 256
MAXL = 3
ROWS = 8
LANES = 128


def split3(x):
    h1 = x.astype(jnp.bfloat16).astype(jnp.float32)
    rest = x - h1
    h2 = rest.astype(jnp.bfloat16).astype(jnp.float32)
    h3 = (rest - h2).astype(jnp.bfloat16).astype(jnp.float32)
    return h1, h2, h3


def coulomb_kernel(ang_ref, gath_ref, coef_ref, core_ref, out_ref, feat_ref, bra_ref, cnt_ref, acc_ref, den0_ref, den1_ref):
    devices, _, width = gath_ref.shape
    own = width // PB
    tiles = LANES
    blocks = devices * own
    me = lax.axis_index("gx")
    first = me * own

    sub = lax.broadcasted_iota(jnp.int32, (blocks, tiles), 0).astype(jnp.float32)

    def count(dev, sums):
        bra = gath_ref[dev, pl.ds(6, 1), pl.ds(0, tiles)]
        ket = gath_ref[dev, pl.ds(6, 1), pl.ds(tiles, tiles)]
        return tuple(
            total + jnp.where(jnp.where(bra == (first + b).astype(jnp.float32), ket, -1.0) == sub, 1.0, 0.0)
            for b, total in enumerate(sums)
        )

    sums = lax.fori_loop(
        0, devices, count, tuple(jnp.zeros((blocks, tiles), jnp.float32) for _ in range(own)), unroll=devices <= 16
    )
    for b in range(own):
        cnt_ref[b] = jnp.broadcast_to(jnp.sum(sums[b], axis=1, keepdims=True), (blocks, LANES))

    def features(dev, carry):
        h1, h2, h3 = split3(gath_ref[dev])
        feat_ref[:, pl.ds(pl.multiple_of(dev * width, width), width)] = jnp.concatenate(
            [h1, h2, h3, h1, h2, h1], axis=0
        ).astype(jnp.bfloat16)
        return carry

    lax.fori_loop(0, devices, features, 0, unroll=4)

    mine = gath_ref[me]
    parts = split3(mine)
    norm = mine[3:4, :]
    row = lax.broadcasted_iota(jnp.int32, mine.shape, 0)
    for which, total in enumerate((norm + mine[4:5, :], norm)):
        consts = split3(total)
        groups = []
        for group, (part, const) in enumerate(((0, 0), (0, None), (0, None), (1, 1), (1, None), (2, 2))):
            value = jnp.where(row < 3, -2.0 * parts[part], 0.0)
            if group < 3:
                value = jnp.where((row == 3) | (row == 4) if which == 0 else row == 3, 1.0, value)
            if const is not None:
                value = jnp.where(row == 7, consts[const], value)
            groups.append(value)
        groups.append(jnp.zeros((LANES - 6 * ROWS, width), jnp.float32))
        turned = jnp.concatenate(groups, axis=0).T
        for b in range(own):
            bra_ref[b, pl.ds(which * PB, PB), :] = turned[b * PB : (b + 1) * PB, : 6 * ROWS].astype(jnp.bfloat16)

    acc_ref[...] = jnp.zeros_like(acc_ref)
    dens = (den0_ref, den1_ref)

    def fill(b, ket):
        dens[b][...] = jnp.dot(
            bra_ref[b],
            feat_ref[:, pl.ds(pl.multiple_of(ket * PB, PB), PB)],
            preferred_element_type=jnp.float32,
        )

    def evaluate(kind, b, ket):
        dev = ket // own
        start = pl.multiple_of((ket - dev * own) * PB, PB)
        times = cnt_ref[b, pl.ds(ket, 1), :] * (1.0 / (2 * kind + 1))
        weight = gath_ref[dev, pl.ds(5, 1), pl.ds(start, PB)] * jnp.concatenate([times] * (PB // LANES), axis=1)
        step = 16
        weight = jnp.broadcast_to(weight, (step, PB))
        for at in range(0, PB, step):
            root = lax.rsqrt(dens[b][pl.ds(at, step), :])
            if kind > 0:
                ratio = dens[b][pl.ds(PB + at, step), :] * root * root
                series = ratio + (2 * kind + 1) / (2 * kind - 1)
                for power in range(kind - 2, -1, -1):
                    series = series * ratio + (2 * kind + 1) / (2 * power + 1)
                root = series * root
            value = root * weight
            total = acc_ref[b, pl.ds(at, step), :]
            for lane in range(0, PB, LANES):
                total = total + value[:, lane : lane + LANES]
            acc_ref[b, pl.ds(at, step), :] = total

    fill(0, 0)

    def one_ket(ket, carry):
        level = ang_ref[ket]
        for b in range(own):
            kind = ang_ref[first + b] + level

            def branch(k, b=b):
                def run():
                    if b + 1 < own:
                        fill(b + 1, ket)
                    else:
                        fill(0, jnp.minimum(ket + 1, blocks - 1))
                    evaluate(k, b, ket)

                return run

            lax.switch(kind, [branch(k) for k in range(2 * MAXL + 1)])
        return carry

    lax.fori_loop(0, blocks, one_ket, 0)
    for b in range(own):
        lanes = pl.ds(b * PB, PB)
        out_ref[:, lanes] = core_ref[:, lanes] + coef_ref[:, lanes] * jnp.sum(acc_ref[b].T, axis=0, keepdims=True)


def shards(coefficient, exponent, centers, density, core_fock, shell_ang, tile_list):
    width = exponent.shape[0]
    own = width // PB
    devices = lax.axis_size("gx")
    blocks = devices * own
    tile_row = jnp.pad(tile_list.astype(jnp.float32).reshape(-1), (0, width - tile_list.size))
    packed = jnp.concatenate(
        [
            centers,
            jnp.sum(centers * centers, axis=0, keepdims=True),
            exponent[None],
            (coefficient * density)[None],
            tile_row[None],
            jnp.ones((1, width), jnp.float32),
        ],
        axis=0,
    )
    gathered = gather(packed, devices)
    out = pl.pallas_call(
        coulomb_kernel,
        out_shape=jax.ShapeDtypeStruct((1, width), jnp.float32),
        in_specs=[pl.BlockSpec(memory_space=pltpu.SMEM)] + [pl.BlockSpec(memory_space=pltpu.VMEM)] * 3,
        out_specs=pl.BlockSpec(memory_space=pltpu.VMEM),
        scratch_shapes=[
            pltpu.VMEM((6 * ROWS, devices * width), jnp.bfloat16),
            pltpu.VMEM((own, 2 * PB, 6 * ROWS), jnp.bfloat16),
            pltpu.VMEM((own, blocks, LANES), jnp.float32),
            pltpu.VMEM((own, PB, LANES), jnp.float32),
            pltpu.VMEM((2 * PB, PB), jnp.float32),
            pltpu.VMEM((2 * PB, PB), jnp.float32),
        ],
        compiler_params=pltpu.CompilerParams(vmem_limit_bytes=40 * 1024 * 1024),
        name="coulomb",
    )(shell_ang, gathered, coefficient[None], core_fock[None])
    return out.reshape(width)


def gather(packed, devices):
    spread = jnp.broadcast_to(packed[None], (devices,) + packed.shape)
    return lax.all_to_all(spread, "gx", split_axis=0, concat_axis=0)


def solution(mesh):
    return jax.shard_map(
        shards,
        mesh=mesh,
        in_specs=(
            P(("frag", "gx")),
            P(("frag", "gx")),
            P(None, ("frag", "gx")),
            P(("frag", "gx")),
            P(("frag", "gx")),
            P("frag"),
            P(None, ("frag", "gx")),
        ),
        out_specs=P(("frag", "gx")),
        check_vma=False,
    )
```

```python
import jax
import jax.numpy as jnp
from jax import lax
from jax.experimental import pallas as pl
from jax.experimental.pallas import tpu as pltpu
from jax.sharding import PartitionSpec as P

PB = 256
MAXL = 3
ROWS = 8
LANES = 128


def split3(x):
    h1 = x.astype(jnp.bfloat16).astype(jnp.float32)
    rest = x - h1
    h2 = rest.astype(jnp.bfloat16).astype(jnp.float32)
    h3 = (rest - h2).astype(jnp.bfloat16).astype(jnp.float32)
    return h1, h2, h3


def pack_kernel(exp_hbm, cen_hbm, coef_hbm, dens_hbm, tile_hbm, out_ref, one_ref, two_ref, cen_ref, tile_ref, row_ref, sems):
    copies = [
        pltpu.make_async_copy(src, dst, sems.at[i])
        for i, (src, dst) in enumerate(
            (
                (exp_hbm, row_ref.at[pl.ds(4, 1)]),
                (cen_hbm, cen_ref),
                (coef_hbm, one_ref),
                (dens_hbm, two_ref),
                (tile_hbm, tile_ref),
            )
        )
    ]
    for copy in copies:
        copy.start()
    for copy in copies:
        copy.wait()
    tiles = tile_ref.shape[1]
    centers = cen_ref[...]
    row_ref[0:3, :] = centers
    row_ref[3:4, :] = jnp.sum(centers * centers, axis=0, keepdims=True)
    row_ref[5:6, :] = one_ref[...] * two_ref[...]
    row_ref[6:8, :] = jnp.ones((2, row_ref.shape[1]), jnp.float32)
    listing = tile_ref[...].astype(jnp.float32)
    row_ref[6:7, 0:tiles] = listing[0:1]
    row_ref[6:7, tiles : 2 * tiles] = listing[1:2]
    packed = row_ref[...]
    for device in range(out_ref.shape[0]):
        out_ref[device] = packed


def prepare_kernel(ang_ref, own_ref, bra_ref, order_ref, next_ref):
    own = own_ref.shape[2] // PB
    blocks = ang_ref.shape[0]
    for level in range(MAXL + 1):
        next_ref[level] = level * (blocks // (MAXL + 1))

    def place(block, carry):
        level = ang_ref[block]
        position = next_ref[level]
        order_ref[position] = block
        next_ref[level] = position + 1
        return carry

    lax.fori_loop(0, blocks, place, 0)

    mine = own_ref[0]
    width = mine.shape[1]
    parts = split3(mine)
    norm = mine[3:4, :]
    row = lax.broadcasted_iota(jnp.int32, mine.shape, 0)
    for which, total in enumerate((norm + mine[4:5, :], norm)):
        consts = split3(total)
        groups = []
        for group, (part, const) in enumerate(((0, 0), (0, None), (0, None), (1, 1), (1, None), (2, 2))):
            value = jnp.where(row < 3, -2.0 * parts[part], 0.0)
            if group < 3:
                value = jnp.where((row == 3) | (row == 4) if which == 0 else row == 3, 1.0, value)
            if const is not None:
                value = jnp.where(row == 7, consts[const], value)
            groups.append(value)
        groups.append(jnp.zeros((LANES - 6 * ROWS, width), jnp.float32))
        turned = jnp.concatenate(groups, axis=0).T
        for b in range(own):
            bra_ref[b, pl.ds(which * PB, PB), :] = turned[b * PB : (b + 1) * PB, : 6 * ROWS].astype(jnp.bfloat16)


def coulomb_kernel(
    ang_ref, order_ref, gath_ref, bra_ref, coef_hbm, core_hbm, out_ref,
    feat_ref, cnt_ref, acc_ref, den0_ref, den1_ref, coef_ref, core_ref, sems,
):
    devices, _, width = gath_ref.shape
    own = width // PB
    tiles = LANES
    blocks = devices * own
    first = lax.axis_index("gx") * own
    late = [
        pltpu.make_async_copy(coef_hbm, coef_ref, sems.at[0]),
        pltpu.make_async_copy(core_hbm, core_ref, sems.at[1]),
    ]
    for copy in late:
        copy.start()

    sub = lax.broadcasted_iota(jnp.int32, (blocks, tiles), 0).astype(jnp.float32)

    def count(dev, sums):
        bra = gath_ref[dev, pl.ds(6, 1), pl.ds(0, tiles)]
        ket = gath_ref[dev, pl.ds(6, 1), pl.ds(tiles, tiles)]
        return tuple(
            total + jnp.where(jnp.where(bra == (first + b).astype(jnp.float32), ket, -1.0) == sub, 1.0, 0.0)
            for b, total in enumerate(sums)
        )

    sums = lax.fori_loop(
        0, devices, count, tuple(jnp.zeros((blocks, tiles), jnp.float32) for _ in range(own)), unroll=devices <= 16
    )
    for b in range(own):
        cnt_ref[b] = jnp.broadcast_to(jnp.sum(sums[b], axis=1, keepdims=True), (blocks, LANES))

    def features(dev, carry):
        h1, h2, h3 = split3(gath_ref[dev])
        feat_ref[:, pl.ds(pl.multiple_of(dev * width, width), width)] = jnp.concatenate(
            [h1, h2, h3, h1, h2, h1], axis=0
        ).astype(jnp.bfloat16)
        return carry

    lax.fori_loop(0, devices, features, 0, unroll=4)
    acc_ref[...] = jnp.zeros_like(acc_ref)
    last = own * blocks - 1
    size = blocks // (MAXL + 1)

    def tile_at(position):
        b = position // blocks
        return b, order_ref[position - b * blocks]

    def fill(den_ref, position):
        b, ket = tile_at(jnp.minimum(position, last))
        den_ref[...] = jnp.dot(
            bra_ref[b],
            feat_ref[:, pl.ds(pl.multiple_of(ket * PB, PB), PB)],
            preferred_element_type=jnp.float32,
        )

    def evaluate(kind, den_ref, position):
        b, ket = tile_at(position)
        dev = ket // own
        start = pl.multiple_of((ket - dev * own) * PB, PB)
        times = cnt_ref[b, pl.ds(ket, 1), :] * (1.0 / (2 * kind + 1))
        weight = gath_ref[dev, pl.ds(5, 1), pl.ds(start, PB)] * jnp.concatenate([times] * (PB // LANES), axis=1)
        step = 16
        weight = jnp.broadcast_to(weight, (step, PB))
        for at in range(0, PB, step):
            root = lax.rsqrt(den_ref[pl.ds(at, step), :])
            if kind > 0:
                ratio = den_ref[pl.ds(PB + at, step), :] * root * root
                series = ratio + (2 * kind + 1) / (2 * kind - 1)
                for power in range(kind - 2, -1, -1):
                    series = series * ratio + (2 * kind + 1) / (2 * power + 1)
                root = series * root
            value = root * weight
            total = acc_ref[b, pl.ds(at, step), :]
            for lane in range(0, PB, LANES):
                total = total + value[:, lane : lane + LANES]
            acc_ref[b, pl.ds(at, step), :] = total

    fill(den0_ref, 0)

    def one_group(group, carry):
        b = group // (MAXL + 1)
        kind = ang_ref[first + b] + group - b * (MAXL + 1)

        def branch(k):
            def run():
                def two_kets(i, carry):
                    position = group * size + 2 * i
                    fill(den1_ref, position + 1)
                    evaluate(k, den0_ref, position)
                    fill(den0_ref, position + 2)
                    evaluate(k, den1_ref, position + 1)
                    return carry

                lax.fori_loop(0, size // 2, two_kets, 0)

            return run

        lax.switch(kind, [branch(k) for k in range(2 * MAXL + 1)])
        return carry

    lax.fori_loop(0, own * (MAXL + 1), one_group, 0)
    for copy in late:
        copy.wait()
    for b in range(own):
        lanes = pl.ds(b * PB, PB)
        out_ref[:, lanes] = core_ref[:, lanes] + coef_ref[:, lanes] * jnp.sum(acc_ref[b].T, axis=0, keepdims=True)


def shards(coefficient, exponent, centers, density, core_fock, shell_ang, tile_list):
    width = exponent.shape[0]
    own = width // PB
    devices = lax.axis_size("gx")
    blocks = devices * own
    anywhere = pl.BlockSpec(memory_space=pltpu.HBM)
    vmem = pl.BlockSpec(memory_space=pltpu.VMEM)
    smem = pl.BlockSpec(memory_space=pltpu.SMEM)
    limits = pltpu.CompilerParams(vmem_limit_bytes=40 * 1024 * 1024)
    row = pltpu.VMEM((1, width), jnp.float32)
    spread = pl.pallas_call(
        pack_kernel,
        out_shape=jax.ShapeDtypeStruct((devices, ROWS, width), jnp.float32),
        in_specs=[anywhere] * 5,
        out_specs=vmem,
        scratch_shapes=[
            row,
            row,
            pltpu.VMEM(centers.shape, jnp.float32),
            pltpu.VMEM(tile_list.shape, jnp.int32),
            pltpu.VMEM((ROWS, width), jnp.float32),
            pltpu.SemaphoreType.DMA((5,)),
        ],
        compiler_params=limits,
        name="pack",
    )(exponent[None], centers, coefficient[None], density[None], tile_list)
    gathered = lax.all_to_all(spread, "gx", split_axis=0, concat_axis=0)
    bra, order = pl.pallas_call(
        prepare_kernel,
        grid=(1,),
        out_shape=(
            jax.ShapeDtypeStruct((own, 2 * PB, 6 * ROWS), jnp.bfloat16),
            jax.ShapeDtypeStruct((blocks,), jnp.int32),
        ),
        in_specs=[smem, pl.BlockSpec((1, ROWS, width), lambda i: (0, 0, 0))],
        out_specs=(vmem, smem),
        scratch_shapes=[pltpu.SMEM((MAXL + 1,), jnp.int32)],
        compiler_params=limits,
        cost_estimate=pl.CostEstimate(flops=10**8, bytes_accessed=10**6, transcendentals=0),
        name="prepare",
    )(shell_ang, spread)
    out = pl.pallas_call(
        coulomb_kernel,
        out_shape=jax.ShapeDtypeStruct((1, width), jnp.float32),
        in_specs=[smem, smem, vmem, vmem, anywhere, anywhere],
        out_specs=vmem,
        scratch_shapes=[
            pltpu.VMEM((6 * ROWS, devices * width), jnp.bfloat16),
            pltpu.VMEM((own, blocks, LANES), jnp.float32),
            pltpu.VMEM((own, PB, LANES), jnp.float32),
            pltpu.VMEM((2 * PB, PB), jnp.float32),
            pltpu.VMEM((2 * PB, PB), jnp.float32),
            row,
            row,
            pltpu.SemaphoreType.DMA((2,)),
        ],
        compiler_params=limits,
        name="coulomb",
    )(shell_ang, order, gathered, bra, coefficient[None], core_fock[None])
    return out.reshape(width)


def solution(mesh):
    return jax.shard_map(
        shards,
        mesh=mesh,
        in_specs=(
            P(("frag", "gx")),
            P(("frag", "gx")),
            P(None, ("frag", "gx")),
            P(("frag", "gx")),
            P(("frag", "gx")),
            P("frag"),
            P(None, ("frag", "gx")),
        ),
        out_specs=P(("frag", "gx")),
        check_vma=False,
    )
```

```python
import jax
import jax.numpy as jnp
from jax import lax
from jax.experimental import pallas as pl
from jax.experimental.pallas import tpu as pltpu
from jax.sharding import PartitionSpec as P

PB = 256
MAXL = 3
ROWS = 8
LANES = 128


def split3(x):
    h1 = x.astype(jnp.bfloat16).astype(jnp.float32)
    rest = x - h1
    h2 = rest.astype(jnp.bfloat16).astype(jnp.float32)
    h3 = (rest - h2).astype(jnp.bfloat16).astype(jnp.float32)
    return h1, h2, h3


def pack_kernel(exp_hbm, cen_hbm, coef_hbm, dens_hbm, tile_hbm, out_ref, one_ref, two_ref, cen_ref, tile_ref, row_ref, sems):
    copies = [
        pltpu.make_async_copy(src, dst, sems.at[i])
        for i, (src, dst) in enumerate(
            (
                (exp_hbm, row_ref.at[pl.ds(4, 1)]),
                (cen_hbm, cen_ref),
                (coef_hbm, one_ref),
                (dens_hbm, two_ref),
                (tile_hbm, tile_ref),
            )
        )
    ]
    for copy in copies:
        copy.start()
    for copy in copies:
        copy.wait()
    tiles = tile_ref.shape[1]
    centers = cen_ref[...]
    row_ref[0:3, :] = centers
    row_ref[3:4, :] = jnp.sum(centers * centers, axis=0, keepdims=True)
    row_ref[5:6, :] = one_ref[...] * two_ref[...]
    row_ref[6:8, :] = jnp.ones((2, row_ref.shape[1]), jnp.float32)
    listing = tile_ref[...].astype(jnp.float32)
    row_ref[6:7, 0:tiles] = listing[0:1]
    row_ref[6:7, tiles : 2 * tiles] = listing[1:2]
    packed = row_ref[...]
    for device in range(out_ref.shape[0]):
        out_ref[device] = packed


def prepare_kernel(ang_ref, own_ref, bra_ref, order_ref, next_ref):
    own = own_ref.shape[2] // PB
    blocks = ang_ref.shape[0]
    for level in range(MAXL + 1):
        next_ref[level] = level * (blocks // (MAXL + 1))

    def place(block, carry):
        level = ang_ref[block]
        position = next_ref[level]
        order_ref[position] = block
        next_ref[level] = position + 1
        return carry

    lax.fori_loop(0, blocks, place, 0)

    mine = own_ref[0]
    width = mine.shape[1]
    parts = split3(mine)
    norm = mine[3:4, :]
    row = lax.broadcasted_iota(jnp.int32, mine.shape, 0)
    for which, total in enumerate((norm + mine[4:5, :], norm)):
        consts = split3(total)
        groups = []
        for group, (part, const) in enumerate(((0, 0), (0, None), (0, None), (1, 1), (1, None), (2, 2))):
            value = jnp.where(row < 3, -2.0 * parts[part], 0.0)
            if group < 3:
                value = jnp.where((row == 3) | (row == 4) if which == 0 else row == 3, 1.0, value)
            if const is not None:
                value = jnp.where(row == 7, consts[const], value)
            groups.append(value)
        groups.append(jnp.zeros((LANES - 6 * ROWS, width), jnp.float32))
        turned = jnp.concatenate(groups, axis=0).T
        for b in range(own):
            bra_ref[b, pl.ds(which * PB, PB), :] = turned[b * PB : (b + 1) * PB, : 6 * ROWS].astype(jnp.bfloat16)


def coulomb_kernel(
    ang_ref, order_ref, gath_ref, bra_ref, coef_hbm, core_hbm, out_ref,
    feat_ref, cnt_ref, acc_ref, den0_ref, den1_ref, coef_ref, core_ref, sems,
):
    devices, _, width = gath_ref.shape
    own = width // PB
    tiles = LANES
    blocks = devices * own
    first = lax.axis_index("gx") * own
    late = [
        pltpu.make_async_copy(coef_hbm, coef_ref, sems.at[0]),
        pltpu.make_async_copy(core_hbm, core_ref, sems.at[1]),
    ]
    for copy in late:
        copy.start()

    sub = lax.broadcasted_iota(jnp.int32, (blocks, tiles), 0).astype(jnp.float32)

    def count(dev, sums):
        bra = gath_ref[dev, pl.ds(6, 1), pl.ds(0, tiles)]
        ket = gath_ref[dev, pl.ds(6, 1), pl.ds(tiles, tiles)]
        return tuple(
            total + jnp.where(jnp.where(bra == (first + b).astype(jnp.float32), ket, -1.0) == sub, 1.0, 0.0)
            for b, total in enumerate(sums)
        )

    sums = lax.fori_loop(
        0, devices, count, tuple(jnp.zeros((blocks, tiles), jnp.float32) for _ in range(own)), unroll=devices <= 16
    )
    for b in range(own):
        cnt_ref[b] = jnp.broadcast_to(jnp.sum(sums[b], axis=1, keepdims=True), (blocks, LANES))

    def features(dev, carry):
        h1, h2, h3 = split3(gath_ref[dev])
        feat_ref[:, pl.ds(pl.multiple_of(dev * width, width), width)] = jnp.concatenate(
            [h1, h2, h3, h1, h2, h1], axis=0
        ).astype(jnp.bfloat16)
        return carry

    lax.fori_loop(0, devices, features, 0, unroll=4)
    acc_ref[...] = jnp.zeros_like(acc_ref)
    last = own * blocks - 1
    size = blocks // (MAXL + 1)

    def tile_at(position):
        b = position // blocks
        return b, order_ref[position - b * blocks]

    def fill(den_ref, position):
        b, ket = tile_at(jnp.minimum(position, last))
        den_ref[...] = jnp.dot(
            bra_ref[b],
            feat_ref[:, pl.ds(pl.multiple_of(ket * PB, PB), PB)],
            preferred_element_type=jnp.float32,
        )

    def evaluate(kind, den_ref, position):
        b, ket = tile_at(position)
        dev = ket // own
        start = pl.multiple_of((ket - dev * own) * PB, PB)
        times = cnt_ref[b, pl.ds(ket, 1), :] * (1.0 / (2 * kind + 1))
        weight = gath_ref[dev, pl.ds(5, 1), pl.ds(start, PB)] * jnp.concatenate([times] * (PB // LANES), axis=1)
        step = 16
        weight = jnp.broadcast_to(weight, (step, PB))
        for at in range(0, PB, step):
            root = lax.rsqrt(den_ref[pl.ds(at, step), :])
            if kind > 0:
                ratio = den_ref[pl.ds(PB + at, step), :] * root * root
                series = ratio + (2 * kind + 1) / (2 * kind - 1)
                for power in range(kind - 2, -1, -1):
                    series = series * ratio + (2 * kind + 1) / (2 * power + 1)
                root = series * root
            value = root * weight
            total = acc_ref[b, pl.ds(at, step), :]
            for lane in range(0, PB, LANES):
                total = total + value[:, lane : lane + LANES]
            acc_ref[b, pl.ds(at, step), :] = total

    fill(den0_ref, 0)

    def one_group(group, carry):
        b = group // (MAXL + 1)
        kind = ang_ref[first + b] + group - b * (MAXL + 1)

        def branch(k):
            def run():
                def two_kets(i, carry):
                    position = group * size + 2 * i
                    fill(den1_ref, position + 1)
                    evaluate(k, den0_ref, position)
                    fill(den0_ref, position + 2)
                    evaluate(k, den1_ref, position + 1)
                    return carry

                lax.fori_loop(0, size // 2, two_kets, 0)

            return run

        lax.switch(kind, [branch(k) for k in range(2 * MAXL + 1)])
        return carry

    lax.fori_loop(0, own * (MAXL + 1), one_group, 0)
    for copy in late:
        copy.wait()
    for b in range(own):
        lanes = pl.ds(b * PB, PB)
        out_ref[:, lanes] = core_ref[:, lanes] + coef_ref[:, lanes] * jnp.sum(acc_ref[b].T, axis=0, keepdims=True)


def shards(coefficient, exponent, centers, density, core_fock, shell_ang, tile_list):
    width = exponent.shape[0]
    own = width // PB
    devices = lax.axis_size("gx")
    blocks = devices * own
    anywhere = pl.BlockSpec(memory_space=pltpu.HBM)
    vmem = pl.BlockSpec(memory_space=pltpu.VMEM)
    smem = pl.BlockSpec(memory_space=pltpu.SMEM)
    limits = pltpu.CompilerParams(vmem_limit_bytes=40 * 1024 * 1024)
    row = pltpu.VMEM((1, width), jnp.float32)
    spread = pl.pallas_call(
        pack_kernel,
        out_shape=jax.ShapeDtypeStruct((devices, ROWS, width), jnp.float32),
        in_specs=[anywhere] * 5,
        out_specs=vmem,
        scratch_shapes=[
            row,
            row,
            pltpu.VMEM(centers.shape, jnp.float32),
            pltpu.VMEM(tile_list.shape, jnp.int32),
            pltpu.VMEM((ROWS, width), jnp.float32),
            pltpu.SemaphoreType.DMA((5,)),
        ],
        compiler_params=limits,
        name="pack",
    )(*[pltpu.with_memory_space_constraint(a, pltpu.HBM) for a in (exponent[None], centers, coefficient[None], density[None], tile_list)])
    gathered = lax.all_to_all(spread, "gx", split_axis=0, concat_axis=0)
    bra, order = pl.pallas_call(
        prepare_kernel,
        grid=(1,),
        out_shape=(
            jax.ShapeDtypeStruct((own, 2 * PB, 6 * ROWS), jnp.bfloat16),
            jax.ShapeDtypeStruct((blocks,), jnp.int32),
        ),
        in_specs=[smem, pl.BlockSpec((1, ROWS, width), lambda i: (0, 0, 0))],
        out_specs=(vmem, smem),
        scratch_shapes=[pltpu.SMEM((MAXL + 1,), jnp.int32)],
        compiler_params=limits,
        cost_estimate=pl.CostEstimate(flops=10**8, bytes_accessed=10**6, transcendentals=0),
        name="prepare",
    )(shell_ang, spread)
    out = pl.pallas_call(
        coulomb_kernel,
        out_shape=jax.ShapeDtypeStruct((1, width), jnp.float32),
        in_specs=[smem, smem, vmem, vmem, anywhere, anywhere],
        out_specs=vmem,
        scratch_shapes=[
            pltpu.VMEM((6 * ROWS, devices * width), jnp.bfloat16),
            pltpu.VMEM((own, blocks, LANES), jnp.float32),
            pltpu.VMEM((own, PB, LANES), jnp.float32),
            pltpu.VMEM((2 * PB, PB), jnp.float32),
            pltpu.VMEM((2 * PB, PB), jnp.float32),
            row,
            row,
            pltpu.SemaphoreType.DMA((2,)),
        ],
        compiler_params=limits,
        name="coulomb",
    )(
        shell_ang, order, gathered, bra, *[pltpu.with_memory_space_constraint(a, pltpu.HBM) for a in (coefficient[None], core_fock[None])]
    )
    return out.reshape(width)


def solution(mesh):
    return jax.shard_map(
        shards,
        mesh=mesh,
        in_specs=(
            P(("frag", "gx")),
            P(("frag", "gx")),
            P(None, ("frag", "gx")),
            P(("frag", "gx")),
            P(("frag", "gx")),
            P("frag"),
            P(None, ("frag", "gx")),
        ),
        out_specs=P(("frag", "gx")),
        check_vma=False,
    )
```

```python
import math

import jax
import jax.numpy as jnp
from jax import lax
from jax.experimental import pallas as pl
from jax.experimental.pallas import tpu as pltpu
from jax.sharding import PartitionSpec as P

PB = 256
MAXL = 3
ROWS = 8
LANES = 128


def series_in_rest(kind):
    return [
        (-1) ** power * sum(math.comb(m, power) / (2 * m + 1) for m in range(power, kind + 1))
        for power in range(kind + 1)
    ]


def split3(x):
    h1 = x.astype(jnp.bfloat16).astype(jnp.float32)
    rest = x - h1
    h2 = rest.astype(jnp.bfloat16).astype(jnp.float32)
    h3 = (rest - h2).astype(jnp.bfloat16).astype(jnp.float32)
    return h1, h2, h3


def pack_kernel(exp_hbm, cen_hbm, coef_hbm, dens_hbm, tile_hbm, out_ref, one_ref, two_ref, cen_ref, tile_ref, row_ref, sems):
    copies = [
        pltpu.make_async_copy(src, dst, sems.at[i])
        for i, (src, dst) in enumerate(
            (
                (exp_hbm, row_ref.at[pl.ds(4, 1)]),
                (cen_hbm, cen_ref),
                (coef_hbm, one_ref),
                (dens_hbm, two_ref),
                (tile_hbm, tile_ref),
            )
        )
    ]
    for copy in copies:
        copy.start()
    for copy in copies:
        copy.wait()
    tiles = tile_ref.shape[1]
    centers = cen_ref[...]
    row_ref[0:3, :] = centers
    row_ref[3:4, :] = jnp.sum(centers * centers, axis=0, keepdims=True)
    row_ref[5:6, :] = one_ref[...] * two_ref[...]
    row_ref[6:8, :] = jnp.ones((2, row_ref.shape[1]), jnp.float32)
    listing = tile_ref[...].astype(jnp.float32)
    row_ref[6:7, 0:tiles] = listing[0:1]
    row_ref[6:7, tiles : 2 * tiles] = listing[1:2]
    packed = row_ref[...]
    for device in range(out_ref.shape[0]):
        out_ref[device] = packed


def prepare_kernel(ang_ref, own_ref, bra_ref, braexp_ref, order_ref, next_ref):
    own = own_ref.shape[2] // PB
    blocks = ang_ref.shape[0]
    for level in range(MAXL + 1):
        next_ref[level] = level * (blocks // (MAXL + 1))

    def place(block, carry):
        level = ang_ref[block]
        position = next_ref[level]
        order_ref[position] = block
        next_ref[level] = position + 1
        return carry

    lax.fori_loop(0, blocks, place, 0)

    mine = own_ref[0]
    width = mine.shape[1]
    parts = split3(mine)
    norm = mine[3:4, :]
    row = lax.broadcasted_iota(jnp.int32, mine.shape, 0)
    consts = split3(norm + mine[4:5, :])
    groups = []
    for group, (part, const) in enumerate(((0, 0), (0, None), (0, None), (1, 1), (1, None), (2, 2))):
        value = jnp.where(row < 3, -2.0 * parts[part], 0.0)
        if group < 3:
            value = jnp.where((row == 3) | (row == 4), 1.0, value)
        if const is not None:
            value = jnp.where(row == 7, consts[const], value)
        groups.append(value)
    groups.append(jnp.zeros((LANES - 6 * ROWS, width), jnp.float32))
    turned = jnp.concatenate(groups, axis=0).T
    column = jnp.broadcast_to(mine[4:5, :], (LANES, width)).T
    for b in range(own):
        bra_ref[b] = turned[b * PB : (b + 1) * PB, : 6 * ROWS].astype(jnp.bfloat16)
        braexp_ref[b] = column[b * PB : (b + 1) * PB]


def coulomb_kernel(
    ang_ref, order_ref, gath_ref, bra_ref, braexp_ref, coef_hbm, core_hbm, out_ref,
    feat_ref, cnt_ref, acc_ref, den0_ref, den1_ref, coef_ref, core_ref, sems,
):
    devices, _, width = gath_ref.shape
    own = width // PB
    tiles = LANES
    blocks = devices * own
    first = lax.axis_index("gx") * own
    late = [
        pltpu.make_async_copy(coef_hbm, coef_ref, sems.at[0]),
        pltpu.make_async_copy(core_hbm, core_ref, sems.at[1]),
    ]
    for copy in late:
        copy.start()

    sub = lax.broadcasted_iota(jnp.int32, (blocks, tiles), 0).astype(jnp.float32)

    def count(dev, sums):
        bra = gath_ref[dev, pl.ds(6, 1), pl.ds(0, tiles)]
        ket = gath_ref[dev, pl.ds(6, 1), pl.ds(tiles, tiles)]
        return tuple(
            total + jnp.where(jnp.where(bra == (first + b).astype(jnp.float32), ket, -1.0) == sub, 1.0, 0.0)
            for b, total in enumerate(sums)
        )

    sums = lax.fori_loop(
        0, devices, count, tuple(jnp.zeros((blocks, tiles), jnp.float32) for _ in range(own)), unroll=devices <= 16
    )
    for b in range(own):
        cnt_ref[b] = jnp.broadcast_to(jnp.sum(sums[b], axis=1, keepdims=True), (blocks, LANES))

    def features(dev, carry):
        h1, h2, h3 = split3(gath_ref[dev])
        feat_ref[:, pl.ds(pl.multiple_of(dev * width, width), width)] = jnp.concatenate(
            [h1, h2, h3, h1, h2, h1], axis=0
        ).astype(jnp.bfloat16)
        return carry

    lax.fori_loop(0, devices, features, 0, unroll=4)
    acc_ref[...] = jnp.zeros_like(acc_ref)
    last = own * blocks - 1
    size = blocks // (MAXL + 1)

    def tile_at(position):
        b = position // blocks
        return b, order_ref[position - b * blocks]

    def fill(den_ref, position):
        b, ket = tile_at(jnp.minimum(position, last))
        den_ref[...] = jnp.dot(
            bra_ref[b],
            feat_ref[:, pl.ds(pl.multiple_of(ket * PB, PB), PB)],
            preferred_element_type=jnp.float32,
        )

    def evaluate(kind, den_ref, position):
        b, ket = tile_at(position)
        dev = ket // own
        start = pl.multiple_of((ket - dev * own) * PB, PB)
        factors = series_in_rest(kind)
        times = cnt_ref[b, pl.ds(ket, 1), :] * factors[kind]
        weight = gath_ref[dev, pl.ds(5, 1), pl.ds(start, PB)] * jnp.concatenate([times] * (PB // LANES), axis=1)
        step = 16
        weight = jnp.broadcast_to(weight, (step, PB))
        ket_exponent = jnp.broadcast_to(gath_ref[dev, pl.ds(4, 1), pl.ds(start, PB)], (step, PB))
        for at in range(0, PB, step):
            root = lax.rsqrt(den_ref[pl.ds(at, step), :])
            if kind > 0:
                own_exponent = jnp.concatenate([braexp_ref[b, pl.ds(at, step), :]] * (PB // LANES), axis=1)
                rest = (own_exponent + ket_exponent) * root * root
                series = rest + factors[kind - 1] / factors[kind]
                for power in range(kind - 2, -1, -1):
                    series = series * rest + factors[power] / factors[kind]
                root = series * root
            value = root * weight
            total = acc_ref[b, pl.ds(at, step), :]
            for lane in range(0, PB, LANES):
                total = total + value[:, lane : lane + LANES]
            acc_ref[b, pl.ds(at, step), :] = total

    fill(den0_ref, 0)

    def one_group(group, carry):
        b = group // (MAXL + 1)
        kind = ang_ref[first + b] + group - b * (MAXL + 1)

        def branch(k):
            def run():
                def two_kets(i, carry):
                    position = group * size + 2 * i
                    fill(den1_ref, position + 1)
                    evaluate(k, den0_ref, position)
                    fill(den0_ref, position + 2)
                    evaluate(k, den1_ref, position + 1)
                    return carry

                lax.fori_loop(0, size // 2, two_kets, 0)

            return run

        lax.switch(kind, [branch(k) for k in range(2 * MAXL + 1)])
        return carry

    lax.fori_loop(0, own * (MAXL + 1), one_group, 0)
    for copy in late:
        copy.wait()
    for b in range(own):
        lanes = pl.ds(b * PB, PB)
        out_ref[:, lanes] = core_ref[:, lanes] + coef_ref[:, lanes] * jnp.sum(acc_ref[b].T, axis=0, keepdims=True)


def shards(coefficient, exponent, centers, density, core_fock, shell_ang, tile_list):
    width = exponent.shape[0]
    own = width // PB
    devices = lax.axis_size("gx")
    blocks = devices * own
    anywhere = pl.BlockSpec(memory_space=pltpu.HBM)
    vmem = pl.BlockSpec(memory_space=pltpu.VMEM)
    smem = pl.BlockSpec(memory_space=pltpu.SMEM)
    limits = pltpu.CompilerParams(vmem_limit_bytes=40 * 1024 * 1024)
    row = pltpu.VMEM((1, width), jnp.float32)
    spread = pl.pallas_call(
        pack_kernel,
        out_shape=jax.ShapeDtypeStruct((devices, ROWS, width), jnp.float32),
        in_specs=[anywhere] * 5,
        out_specs=vmem,
        scratch_shapes=[
            row,
            row,
            pltpu.VMEM(centers.shape, jnp.float32),
            pltpu.VMEM(tile_list.shape, jnp.int32),
            pltpu.VMEM((ROWS, width), jnp.float32),
            pltpu.SemaphoreType.DMA((5,)),
        ],
        compiler_params=limits,
        name="pack",
    )(*[pltpu.with_memory_space_constraint(a, pltpu.HBM) for a in (exponent[None], centers, coefficient[None], density[None], tile_list)])
    gathered = lax.all_to_all(spread, "gx", split_axis=0, concat_axis=0)
    bra, bra_exponent, order = pl.pallas_call(
        prepare_kernel,
        grid=(1,),
        out_shape=(
            jax.ShapeDtypeStruct((own, PB, 6 * ROWS), jnp.bfloat16),
            jax.ShapeDtypeStruct((own, PB, LANES), jnp.float32),
            jax.ShapeDtypeStruct((blocks,), jnp.int32),
        ),
        in_specs=[smem, pl.BlockSpec((1, ROWS, width), lambda i: (0, 0, 0))],
        out_specs=(vmem, vmem, smem),
        scratch_shapes=[pltpu.SMEM((MAXL + 1,), jnp.int32)],
        compiler_params=limits,
        cost_estimate=pl.CostEstimate(flops=10**8, bytes_accessed=10**6, transcendentals=0),
        name="prepare",
    )(shell_ang, spread)
    out = pl.pallas_call(
        coulomb_kernel,
        out_shape=jax.ShapeDtypeStruct((1, width), jnp.float32),
        in_specs=[smem, smem, vmem, vmem, vmem, anywhere, anywhere],
        out_specs=vmem,
        scratch_shapes=[
            pltpu.VMEM((6 * ROWS, devices * width), jnp.bfloat16),
            pltpu.VMEM((own, blocks, LANES), jnp.float32),
            pltpu.VMEM((own, PB, LANES), jnp.float32),
            pltpu.VMEM((PB, PB), jnp.float32),
            pltpu.VMEM((PB, PB), jnp.float32),
            row,
            row,
            pltpu.SemaphoreType.DMA((2,)),
        ],
        compiler_params=limits,
        name="coulomb",
    )(
        shell_ang, order, gathered, bra, bra_exponent, *[pltpu.with_memory_space_constraint(a, pltpu.HBM) for a in (coefficient[None], core_fock[None])]
    )
    return out.reshape(width)


def solution(mesh):
    return jax.shard_map(
        shards,
        mesh=mesh,
        in_specs=(
            P(("frag", "gx")),
            P(("frag", "gx")),
            P(None, ("frag", "gx")),
            P(("frag", "gx")),
            P(("frag", "gx")),
            P("frag"),
            P(None, ("frag", "gx")),
        ),
        out_specs=P(("frag", "gx")),
        check_vma=False,
    )
```

```python
import math

import jax
import jax.numpy as jnp
from jax import lax
from jax.experimental import pallas as pl
from jax.experimental.pallas import tpu as pltpu
from jax.sharding import PartitionSpec as P

PB = 256
MAXL = 3
ROWS = 8
LANES = 128


def series_in_rest(kind):
    return [
        (-1) ** power * sum(math.comb(m, power) / (2 * m + 1) for m in range(power, kind + 1))
        for power in range(kind + 1)
    ]


def split3(x):
    h1 = x.astype(jnp.bfloat16).astype(jnp.float32)
    rest = x - h1
    h2 = rest.astype(jnp.bfloat16).astype(jnp.float32)
    h3 = (rest - h2).astype(jnp.bfloat16).astype(jnp.float32)
    return h1, h2, h3


def pack_kernel(exp_hbm, cen_hbm, coef_hbm, dens_hbm, tile_hbm, out_ref, one_ref, two_ref, cen_ref, tile_ref, row_ref, sems):
    copies = [
        pltpu.make_async_copy(src, dst, sems.at[i])
        for i, (src, dst) in enumerate(
            (
                (exp_hbm, row_ref.at[pl.ds(4, 1)]),
                (cen_hbm, cen_ref),
                (coef_hbm, one_ref),
                (dens_hbm, two_ref),
                (tile_hbm, tile_ref),
            )
        )
    ]
    for copy in copies:
        copy.start()
    for copy in copies:
        copy.wait()
    tiles = tile_ref.shape[1]
    centers = cen_ref[...]
    row_ref[0:3, :] = centers
    row_ref[3:4, :] = jnp.sum(centers * centers, axis=0, keepdims=True)
    row_ref[5:6, :] = one_ref[...] * two_ref[...]
    row_ref[6:8, :] = jnp.ones((2, row_ref.shape[1]), jnp.float32)
    listing = tile_ref[...].astype(jnp.float32)
    row_ref[6:7, 0:tiles] = listing[0:1]
    row_ref[6:7, tiles : 2 * tiles] = listing[1:2]
    packed = row_ref[...]
    for device in range(out_ref.shape[0]):
        out_ref[device] = packed


def prepare_kernel(ang_ref, own_ref, bra_ref, braexp_ref, order_ref, next_ref):
    own = own_ref.shape[2] // PB
    blocks = ang_ref.shape[0]
    for level in range(MAXL + 1):
        next_ref[level] = level * (blocks // (MAXL + 1))

    def place(block, carry):
        level = ang_ref[block]
        position = next_ref[level]
        order_ref[position] = block
        next_ref[level] = position + 1
        return carry

    lax.fori_loop(0, blocks, place, 0)

    mine = own_ref[0]
    width = mine.shape[1]
    parts = split3(mine)
    norm = mine[3:4, :]
    row = lax.broadcasted_iota(jnp.int32, mine.shape, 0)
    consts = split3(norm + mine[4:5, :])
    groups = []
    for group, (part, const) in enumerate(((0, 0), (0, None), (0, None), (1, 1), (1, None), (2, 2))):
        value = jnp.where(row < 3, -2.0 * parts[part], 0.0)
        if group < 3:
            value = jnp.where((row == 3) | (row == 4), 1.0, value)
        if const is not None:
            value = jnp.where(row == 7, consts[const], value)
        groups.append(value)
    groups.append(jnp.zeros((LANES - 6 * ROWS, width), jnp.float32))
    turned = jnp.concatenate(groups, axis=0).T
    column = jnp.broadcast_to(mine[4:5, :], (LANES, width)).T
    for b in range(own):
        bra_ref[b] = turned[b * PB : (b + 1) * PB, : 6 * ROWS].astype(jnp.bfloat16)
        braexp_ref[b] = column[b * PB : (b + 1) * PB]


def coulomb_kernel(
    ang_ref, order_ref, gath_ref, bra_ref, braexp_ref, coef_hbm, core_hbm, out_ref,
    feat_ref, cnt_ref, acc_ref, den0_ref, den1_ref, coef_ref, core_ref, sems,
):
    devices, _, width = gath_ref.shape
    own = width // PB
    tiles = LANES
    blocks = devices * own
    first = lax.axis_index("gx") * own
    late = [
        pltpu.make_async_copy(coef_hbm, coef_ref, sems.at[0]),
        pltpu.make_async_copy(core_hbm, core_ref, sems.at[1]),
    ]
    for copy in late:
        copy.start()

    sub = lax.broadcasted_iota(jnp.int32, (blocks, tiles), 0).astype(jnp.float32)

    def count(dev, sums):
        bra = gath_ref[dev, pl.ds(6, 1), pl.ds(0, tiles)]
        ket = gath_ref[dev, pl.ds(6, 1), pl.ds(tiles, tiles)]
        return tuple(
            total + jnp.where(jnp.where(bra == (first + b).astype(jnp.float32), ket, -1.0) == sub, 1.0, 0.0)
            for b, total in enumerate(sums)
        )

    sums = lax.fori_loop(
        0, devices, count, tuple(jnp.zeros((blocks, tiles), jnp.float32) for _ in range(own)), unroll=devices <= 16
    )
    for b in range(own):
        cnt_ref[b] = jnp.broadcast_to(jnp.sum(sums[b], axis=1, keepdims=True), (blocks, LANES))

    def features(dev, carry):
        h1, h2, h3 = split3(gath_ref[dev])
        feat_ref[:, pl.ds(pl.multiple_of(dev * width, width), width)] = jnp.concatenate(
            [h1, h2, h3, h1, h2, h1], axis=0
        ).astype(jnp.bfloat16)
        return carry

    lax.fori_loop(0, devices, features, 0, unroll=4)
    acc_ref[...] = jnp.zeros_like(acc_ref)
    last = own * blocks - 1
    size = blocks // (MAXL + 1)

    def tile_at(position):
        b = position // blocks
        return b, order_ref[position - b * blocks]

    def fill(den_ref, position):
        b, ket = tile_at(jnp.minimum(position, last))
        den_ref[...] = jnp.dot(
            bra_ref[b],
            feat_ref[:, pl.ds(pl.multiple_of(ket * PB, PB), PB)],
            preferred_element_type=jnp.float32,
        )

    def evaluate(kind, den_ref, position):
        b, ket = tile_at(position)
        dev = ket // own
        start = pl.multiple_of((ket - dev * own) * PB, PB)
        factors = series_in_rest(kind)
        times = cnt_ref[b, pl.ds(ket, 1), :] * factors[kind]
        weight = gath_ref[dev, pl.ds(5, 1), pl.ds(start, PB)] * jnp.concatenate([times] * (PB // LANES), axis=1)
        step = 16
        weight = jnp.broadcast_to(weight, (step, PB))
        ket_exponent = jnp.broadcast_to(gath_ref[dev, pl.ds(4, 1), pl.ds(start, PB)], (step, PB))
        for at in range(0, PB, step):
            root = lax.rsqrt(den_ref[pl.ds(at, step), :])
            if kind > 0:
                own_exponent = jnp.concatenate([braexp_ref[b, pl.ds(at, step), :]] * (PB // LANES), axis=1)
                rest = (own_exponent + ket_exponent) * root * root
                series = rest + factors[kind - 1] / factors[kind]
                for power in range(kind - 2, -1, -1):
                    series = series * rest + factors[power] / factors[kind]
                root = series * root
            value = root * weight
            total = acc_ref[b, pl.ds(at, step), :]
            for lane in range(0, PB, LANES):
                total = total + value[:, lane : lane + LANES]
            acc_ref[b, pl.ds(at, step), :] = total

    fill(den0_ref, 0)

    def one_group(group, carry):
        b = group // (MAXL + 1)
        kind = ang_ref[first + b] + group - b * (MAXL + 1)

        def branch(k):
            def run():
                def two_kets(i, carry):
                    position = group * size + 2 * i
                    fill(den1_ref, position + 1)
                    evaluate(k, den0_ref, position)
                    fill(den0_ref, position + 2)
                    evaluate(k, den1_ref, position + 1)
                    return carry

                lax.fori_loop(0, size // 2, two_kets, 0, unroll=2)

            return run

        lax.switch(kind, [branch(k) for k in range(2 * MAXL + 1)])
        return carry

    lax.fori_loop(0, own * (MAXL + 1), one_group, 0)
    for copy in late:
        copy.wait()
    for b in range(own):
        lanes = pl.ds(b * PB, PB)
        out_ref[:, lanes] = core_ref[:, lanes] + coef_ref[:, lanes] * jnp.sum(acc_ref[b].T, axis=0, keepdims=True)


def shards(coefficient, exponent, centers, density, core_fock, shell_ang, tile_list):
    width = exponent.shape[0]
    own = width // PB
    devices = lax.axis_size("gx")
    blocks = devices * own
    anywhere = pl.BlockSpec(memory_space=pltpu.HBM)
    vmem = pl.BlockSpec(memory_space=pltpu.VMEM)
    smem = pl.BlockSpec(memory_space=pltpu.SMEM)
    limits = pltpu.CompilerParams(vmem_limit_bytes=40 * 1024 * 1024)
    row = pltpu.VMEM((1, width), jnp.float32)
    spread = pl.pallas_call(
        pack_kernel,
        out_shape=jax.ShapeDtypeStruct((devices, ROWS, width), jnp.float32),
        in_specs=[anywhere] * 5,
        out_specs=vmem,
        scratch_shapes=[
            row,
            row,
            pltpu.VMEM(centers.shape, jnp.float32),
            pltpu.VMEM(tile_list.shape, jnp.int32),
            pltpu.VMEM((ROWS, width), jnp.float32),
            pltpu.SemaphoreType.DMA((5,)),
        ],
        compiler_params=limits,
        name="pack",
    )(*[pltpu.with_memory_space_constraint(a, pltpu.HBM) for a in (exponent[None], centers, coefficient[None], density[None], tile_list)])
    gathered = lax.all_to_all(spread, "gx", split_axis=0, concat_axis=0)
    bra, bra_exponent, order = pl.pallas_call(
        prepare_kernel,
        grid=(1,),
        out_shape=(
            jax.ShapeDtypeStruct((own, PB, 6 * ROWS), jnp.bfloat16),
            jax.ShapeDtypeStruct((own, PB, LANES), jnp.float32),
            jax.ShapeDtypeStruct((blocks,), jnp.int32),
        ),
        in_specs=[smem, pl.BlockSpec((1, ROWS, width), lambda i: (0, 0, 0))],
        out_specs=(vmem, vmem, smem),
        scratch_shapes=[pltpu.SMEM((MAXL + 1,), jnp.int32)],
        compiler_params=limits,
        cost_estimate=pl.CostEstimate(flops=10**8, bytes_accessed=10**6, transcendentals=0),
        name="prepare",
    )(shell_ang, spread)
    out = pl.pallas_call(
        coulomb_kernel,
        out_shape=jax.ShapeDtypeStruct((1, width), jnp.float32),
        in_specs=[smem, smem, vmem, vmem, vmem, anywhere, anywhere],
        out_specs=vmem,
        scratch_shapes=[
            pltpu.VMEM((6 * ROWS, devices * width), jnp.bfloat16),
            pltpu.VMEM((own, blocks, LANES), jnp.float32),
            pltpu.VMEM((own, PB, LANES), jnp.float32),
            pltpu.VMEM((PB, PB), jnp.float32),
            pltpu.VMEM((PB, PB), jnp.float32),
            row,
            row,
            pltpu.SemaphoreType.DMA((2,)),
        ],
        compiler_params=limits,
        name="coulomb",
    )(
        shell_ang, order, gathered, bra, bra_exponent, *[pltpu.with_memory_space_constraint(a, pltpu.HBM) for a in (coefficient[None], core_fock[None])]
    )
    return out.reshape(width)


def solution(mesh):
    return jax.shard_map(
        shards,
        mesh=mesh,
        in_specs=(
            P(("frag", "gx")),
            P(("frag", "gx")),
            P(None, ("frag", "gx")),
            P(("frag", "gx")),
            P(("frag", "gx")),
            P("frag"),
            P(None, ("frag", "gx")),
        ),
        out_specs=P(("frag", "gx")),
        check_vma=False,
    )
```
